32 devices in a mesh: img: 4 (over x, core), head: 2 (over y), txt: 4 (over z).
Axes of the slice: x: 2, y: 2, z: 4, core: 2. Of those that a mesh axis runs over, the one named last changes fastest.
Arguments:
- image_feats: bfloat16 [4096, 7680], P(('img', 'txt'), 'head'), may hold values from -6 to 6
- key_weight: bfloat16 [7680, 512], P('head'), may hold values from -0.0625 to 0.0625
- value_weight: bfloat16 [7680, 512], P('head'), may hold values from -0.0625 to 0.0625
- queries: bfloat16 [1024, 4096], P('txt', 'head'), may hold values from -21 to 21
- grad_out: bfloat16 [1024, 4096], P('txt', 'head'), may hold values from -768 to 768
- tile_image: int32 [32], P('img'), may hold values from 0 to 7, never falling along the last dimension, each value on 1 to 8 neighbouring positions
- text_sees: int32 [8, 8], replicated, may hold values from 0 to 1, as said below
Outputs:
- attn_out: bfloat16 [1024, 4096], P('txt', 'head')
- grad_feats: bfloat16 [4096, 7680], P(('img', 'txt'), 'head')
The draws below stay inside these ranges and needn't reach their ends.
Inputs may be any that keep to these rules, and one draw needn't show every extreme that they name: `text_sees`: every row holds at least one 1.
All inputs are finite; a program needn't handle non-finite values.
Results may differ from the reference program's by a relative error of at most 0.012.
The reference program's roundings to bfloat16 on the way (of `weights`) count: a program that leaves them out, or rounds other values in their place, can miss the bound.
Values may be sent and summed in bfloat16 or wider, within the bound.
A program may use at most 128 MiB of HBM per device.

```python
import math
import jax
import jax.numpy as jnp
import numpy as np
from jax import lax

DV = 7680
HD = 128
KVH = 4
QH = 32
TILE = 128
TBLK = 128
IMAGES = 8
IMG = 4096
TXT = 1024
TILES = 32
TBLKS = 8
MOST = 8


def draw_queries(key, part):
    key_base, key_scale = jax.random.split(key, 2)
    shape = (TXT, QH * HD)
    row_scale = jnp.exp(jax.random.uniform(key_scale, (TXT, 1), jnp.float32, math.log(0.5), math.log(4.0)))
    base_values = jnp.clip(jax.random.normal(key_base, shape, jnp.float32), -4.0, 4.0)
    return (base_values * row_scale).astype(jnp.bfloat16)


def draw_text_sees(key, part):
    random_bits = jax.random.randint(key, (TBLKS, IMAGES), 0, 2)
    forced = jax.random.randint(jax.random.fold_in(key, 1), (TBLKS, 1), 0, IMAGES)
    forced_hit = (jnp.arange(IMAGES)[None, :] == forced).astype(jnp.int32)
    return jnp.maximum(random_bits, forced_hit).astype(jnp.int32)


def block_scale(own_key, dims, pieces, low, high):
    def one(axis_at, parts):
        steps = jax.random.uniform(jax.random.fold_in(jax.random.fold_in(own_key, 6), axis_at), (parts,), jnp.float32, low / len(pieces), high / len(pieces))
        return jnp.repeat(jnp.exp(steps), dims[axis_at] // parts).reshape((-1,) + (1,) * (len(dims) - axis_at - 1))

    loudness = one(*pieces[0])
    for cut in pieces[1:]:
        loudness = loudness * one(*cut)
    return loudness


def profile(count, total, limit, lean):
    weights = [(1 << 20) // math.isqrt(rank ** lean) + 1 for rank in range(2, count + 1)]
    surplus, counts = total - limit - (count - 1), [1] * (count - 1)
    while surplus > 0:
        movable = [i for i in range(count - 1) if counts[i] < limit]
        pool, remaining = sum([weights[i] for i in movable]), surplus
        for i in movable:
            more = min(limit - counts[i], max(1, remaining * weights[i] // pool), surplus)
            counts[i] = counts[i] + more
            surplus = surplus - more
    return np.array([limit] + counts)


def ragged_sizes(key, number_of, total, most, slope):
    if number_of == 2:
        one = jax.random.randint(key, (), max(1, total - most), min(most, total - 1) + 1)
        return jnp.stack([one, total - one])
    lengths = jnp.asarray(profile(number_of, total, most, slope), jnp.int32)
    pairs = (number_of - 1) // 2
    giver, sink = lengths[1:1 + 2 * pairs:2], lengths[2:2 + 2 * pairs:2]
    slack = jnp.minimum(giver - 1, most - sink)
    moved = jax.random.randint(jax.random.fold_in(key, 1), (pairs,), 0, 1 << 20) % (slack + 1)
    lengths = lengths.at[1:1 + 2 * pairs:2].set(giver - moved).at[2:2 + 2 * pairs:2].set(sink + moved)
    return lengths[jax.random.permutation(jax.random.fold_in(key, 2), number_of)]


def scatter_about(key, dims, deviation, limit, shards=(), kind=jnp.bfloat16):
    loudness = block_scale(key, dims, shards, -0.22, 0.18) if shards else 1.0
    values = jax.random.normal(key, dims, jnp.float32) * deviation * loudness
    return jnp.minimum(jnp.maximum(values, -limit), limit).astype(kind)


def setup_inputs(seed: int = 0) -> dict:
    splits = jax.random.split(jax.random.key(seed), 8)
    image_feats = scatter_about(splits[0], (IMG, DV), 1.0, 6.0, ((0, 16), (1, 2)))
    key_weight = scatter_about(splits[1], (DV, KVH * HD), DV ** -0.5, 0.0625, ((0, 2),))
    value_weight = scatter_about(splits[2], (DV, KVH * HD), DV ** -0.5, 0.0625, ((0, 2),))
    queries = draw_queries(jax.random.fold_in(splits[7], 71), 0)
    grad_out = scatter_about(splits[4], (TXT, QH * HD), 128.0, 768.0, ((0, 4), (1, 2)))
    tile_image = jnp.searchsorted(jnp.cumsum(ragged_sizes(splits[5], IMAGES, TILES, MOST, 2)), jnp.arange(TILES), side="right").astype(jnp.int32)
    text_sees = draw_text_sees(jax.random.fold_in(splits[7], 71), 0)
    return dict(image_feats=image_feats, key_weight=key_weight, value_weight=value_weight, queries=queries, grad_out=grad_out, tile_image=tile_image, text_sees=text_sees)


def attend_one(query, grad_head, key_head, value_head, allowed, scale_factor):
    scores = jnp.dot(query, key_head.T, preferred_element_type=jnp.float32) * scale_factor
    masked = jnp.where(allowed, scores, -1e+30)
    row_max = lax.optimization_barrier(jnp.max(masked, axis=1))
    weights = jnp.exp(masked - row_max[:, None]).astype(jnp.bfloat16)
    totals = lax.optimization_barrier(jnp.sum(weights, axis=1, dtype=jnp.float32))
    numerator = jnp.dot(weights, value_head, preferred_element_type=jnp.float32)
    output = (numerator / totals[:, None]).astype(jnp.bfloat16)
    log_total = row_max + jnp.log(totals)
    row_delta = lax.optimization_barrier(jnp.sum(grad_head.astype(jnp.float32) * output.astype(jnp.float32), axis=1))
    probabilities = jnp.exp(masked - log_total[:, None])
    grad_probs = jnp.dot(grad_head, value_head.T, preferred_element_type=jnp.float32)
    grad_scores = (probabilities * (grad_probs - row_delta[:, None]) * scale_factor).astype(jnp.bfloat16)
    value_grad = jnp.dot(probabilities.astype(jnp.bfloat16).T, grad_head, preferred_element_type=jnp.float32)
    key_grad = jnp.dot(grad_scores.T, query, preferred_element_type=jnp.float32)
    return (output, key_grad, value_grad)

def reference(image_feats, key_weight, value_weight, queries, grad_out, tile_image, text_sees):
    scale_factor = 1.0 / math.sqrt(HD)
    keys = jnp.dot(image_feats, key_weight, preferred_element_type=jnp.float32).astype(jnp.bfloat16)
    values = jnp.dot(image_feats, value_weight, preferred_element_type=jnp.float32).astype(jnp.bfloat16)
    block_allowed = text_sees[:, tile_image]
    allowed = jnp.repeat(jnp.repeat(block_allowed, TBLK, axis=0), TILE, axis=1) > 0
    repeats = QH // KVH
    query_heads = queries.reshape(TXT, KVH, repeats, HD).transpose(1, 2, 0, 3)
    grad_heads = grad_out.reshape(TXT, KVH, repeats, HD).transpose(1, 2, 0, 3)
    key_heads = keys.reshape(IMG, KVH, HD).transpose(1, 0, 2)
    value_heads = values.reshape(IMG, KVH, HD).transpose(1, 0, 2)

    def per_group(operands):
        group_queries, group_grads, key_head, value_head = operands

        def per_query(carry, pair):
            output, key_grad, value_grad = attend_one(pair[0], pair[1], key_head, value_head, allowed, scale_factor)
            return ((carry[0] + key_grad, carry[1] + value_grad), output)
        start = (jnp.zeros((IMG, HD), jnp.float32), jnp.zeros((IMG, HD), jnp.float32))
        summed, outputs = lax.scan(per_query, start, (group_queries, group_grads))
        return (outputs, summed[0], summed[1])
    outputs, key_grad, value_grad = lax.map(per_group, (query_heads, grad_heads, key_heads, value_heads))
    attn_out = outputs.transpose(2, 0, 1, 3).reshape(TXT, QH * HD)
    key_grad = key_grad.transpose(1, 0, 2).reshape(IMG, KVH * HD).astype(jnp.bfloat16)
    value_grad = value_grad.transpose(1, 0, 2).reshape(IMG, KVH * HD).astype(jnp.bfloat16)
    grad_feats = jnp.dot(key_grad, key_weight.T, preferred_element_type=jnp.float32)
    grad_feats = grad_feats + jnp.dot(value_grad, value_weight.T, preferred_element_type=jnp.float32)
    return (attn_out, grad_feats.astype(jnp.bfloat16))
```

```python
import functools
import math

import jax
import jax.numpy as jnp
from jax import lax
from jax.experimental import pallas as pl
from jax.experimental.pallas import tpu as pltpu
from jax.sharding import PartitionSpec as P

HD = 128
TILE = 128
TBLK = 128
MESH = pl.DeviceIdType.MESH
UNROLL = 4
LOG2E = 1.4426950408889634
NT = (((1,), (1,)), ((), ()))
F32 = jnp.float32
BF16 = jnp.bfloat16
HIDE = 2e30
FLOOR = -1e30
ONES = 16
VMEM_BUDGET = 58 * 1024 * 1024


def pick(index, table):
    value = jnp.int32(table[0])
    for at in range(1, len(table)):
        value = jnp.where(index == at, jnp.int32(table[at]), value)
    return value


def arrival_order(count):
    return [
        sorted((b for b in range(count) if b != z), key=lambda b: (abs(b - z), b))
        for z in range(count)
    ]


def departure_order(count):
    orders = []
    for z in range(count):
        above, below = list(range(count - 1, z, -1)), list(range(z))
        orders.append((above + below if 2 * z < count else below + above[::-1]) + [z])
    return orders


def kernel(
    sizes, keep,
    feats_hbm, kw_hbm, vw_hbm, q_hbm, g_hbm, tile_image, text_sees,
    attn, dfeats,
    feats, kw, vw, qraw, graw, qt, gt, big, psend, precv, pacc, kvbuf, vtb, sbuf, numt, mst, tst,
    stbuf, lse, dlt, cown, gsend, grecv, gpart, hall, ocr, xs, xr,
    l_s, w_s, p_ss, p_rs, kv_ss, kv_fs, kv_rs, st_ss, st_rs, oc_ss, oc_rs, ox_ss, ox_rs,
    oa_ss, oa_rs, g_ss, g_rs, h_ss, h_rs,
):
    ni, nh, nt = sizes
    img, hd, txt = lax.axis_index("img"), lax.axis_index("head"), lax.axis_index("txt")
    rows, width = feats.shape
    groups = kvbuf.shape[0]
    own_cols = groups * HD
    text = qraw.shape[0]
    heads = qraw.shape[1] // HD
    reps = heads // groups
    block_tiles = rows // TILE
    scale = 1.0 / math.sqrt(HD)
    unroll = math.gcd(UNROLL, reps)
    half = text // 2
    gcols = reps * HD
    bits = ni.bit_length() - 1
    arrive, depart = arrival_order(nt), departure_order(nt)

    def cols_of(owner, group):
        return pl.ds(pl.multiple_of(owner * own_cols + group * HD, HD), HD)

    def other(step):
        return lax.rem(hd + step, nh)

    loads = [pltpu.make_async_copy(feats_hbm, feats, l_s.at[0])]
    weight_loads = {}
    for step in list(range(1, nh)) + [0]:
        for group in range(groups):
            cols = cols_of(other(step), group)
            pair = [
                pltpu.make_async_copy(src.at[:, cols], dst.at[:, cols], w_s.at[step, group, part])
                for part, (src, dst) in enumerate(((kw_hbm, kw), (vw_hbm, vw)))
            ]
            weight_loads[step, group] = pair
            loads += pair
    q_load = pltpu.make_async_copy(q_hbm, qraw, l_s.at[1])
    g_load = pltpu.make_async_copy(g_hbm, graw, l_s.at[2])
    loads += [q_load, g_load]
    for copy in loads:
        copy.start()

    barrier = pltpu.get_barrier_semaphore()
    for step in range(1, nh):
        pl.semaphore_signal(barrier, inc=1, device_id={"head": other(step)}, device_id_type=MESH)
    for step in range(1, nt):
        pl.semaphore_signal(barrier, inc=1, device_id={"txt": lax.rem(txt + step, nt)}, device_id_type=MESH)
    for step in range(1, ni):
        pl.semaphore_signal(barrier, inc=1, device_id={"img": lax.rem(img + step, ni)}, device_id_type=MESH)

    def remote(src, dst, ss, rs, axis, index):
        return pltpu.make_async_remote_copy(
            src_ref=src, dst_ref=dst, send_sem=ss, recv_sem=rs,
            device_id={axis: index}, device_id_type=MESH,
        )

    first_block = txt * (text // TBLK)
    for tile in range(big.shape[0]):
        image = tile_image[tile]
        parts = [
            jnp.full((1, TBLK), text_sees[first_block + at, image].astype(F32))
            for at in range(text // TBLK)
        ]
        seen = jnp.concatenate(parts, axis=1)
        big[pl.ds(tile, 1), :] = jnp.where(seen > 0.5, 0.0, HIDE)
    vtb[pl.ds(HD, ONES), :] = jnp.ones((ONES, rows), BF16)

    def project(step, group):
        for copy in weight_loads[step, group]:
            copy.wait()
        cols = cols_of(other(step), group)
        weights = jnp.concatenate([kw[:, cols], vw[:, cols]], axis=1)
        return jnp.dot(feats[...], weights, preferred_element_type=F32)

    loads[0].wait()
    p_copies = {}
    for step in range(1, nh):
        for group in range(groups):
            value = project(step, group).astype(BF16)
            if step == 1 and group == 0:
                pl.semaphore_wait(barrier, nh - 1 + nt - 1 + ni - 1)
            for part in range(2):
                psend[step - 1, group, part] = value[:, part * HD : (part + 1) * HD]
                at = (step - 1, group, part)
                copy = remote(
                    psend.at[at], precv.at[at], p_ss.at[at], p_rs.at[at], "head", other(step)
                )
                copy.start()
                p_copies[at] = copy
    for group in range(groups):
        pacc[group] = project(0, group)

    def kv_copy(group, part, side):
        mine = kvbuf.at[group, txt, part]
        return remote(
            mine, mine, kv_ss.at[group, part, side], kv_rs.at[group, txt, part],
            "txt", txt + (1, -1)[side],
        )

    has_side = (txt < nt - 1, txt > 0)

    def own_sum(group, part):
        total = pacc[group, :, part * HD : (part + 1) * HD]
        for step in range(1, nh):
            p_copies[step - 1, group, part].wait_recv()
            total = total + precv[step - 1, group, part].astype(F32)
        kvbuf[group, txt, part] = total.astype(BF16)

    last_pass = [
        [max([0] + [s + 1 for s, b in enumerate(arrive[z]) if (b < z) == (side == 0)]) for z in range(nt)]
        for side in range(2)
    ]

    def send_own(group, after):
        for side in range(2):
            now = has_side[side]
            if after is not None:
                now = jnp.logical_and(now, pick(txt, last_pass[side]) == after)

            def go(side=side):
                for part in range(2):
                    kv_copy(group, part, side).start()

            pl.when(now)(go)

    def arrival(group, step):
        block = pick(txt, [arrive[z][step - 1] for z in range(nt)])
        onward = jnp.where(block < txt, txt + 1, txt - 1)
        valid = jnp.logical_and(onward >= 0, onward < nt)
        copies = []
        for part in range(2):
            there = kvbuf.at[group, block, part]
            copies.append(
                remote(
                    there, there, kv_fs.at[group, step, part], kv_rs.at[group, block, part],
                    "txt", onward,
                )
            )
        return block, valid, copies

    def receive(group, step):
        _, valid, copies = arrival(group, step)
        for copy in copies:
            copy.wait_recv()
            pl.when(valid)(copy.start)

    def turn_over(group):
        def body(at, _):
            head = group * reps + at
            cols = pl.ds(pl.multiple_of(head * HD, HD), HD)
            qt[head] = qraw[:, cols].astype(F32).T.astype(BF16)
            gt[head] = graw[:, cols].astype(F32).T.astype(BF16)
            return 0

        lax.fori_loop(0, reps, body, 0)

    def scaled_scores(keys, head):
        return jnp.dot(keys, qt[head], preferred_element_type=F32) * (scale * LOG2E)

    def tiles_of(array):
        return [array[t * TILE : (t + 1) * TILE] for t in range(block_tiles)]

    def slot(group, block, at):
        return (group * nt + block) * reps + at

    def forward(group, block, first):
        vtb[pl.ds(0, HD), :] = kvbuf[group, block, 1].astype(F32).T.astype(BF16)

        def body(turn, _):
            at = [turn * unroll + i for i in range(unroll)]
            keys, values_t = kvbuf[group, block, 0], vtb[...]
            hide = [big[pl.ds(block * block_tiles + t, 1), :] for t in range(block_tiles)]
            kept, tops, totals, outs = [], [], [], []
            for i in range(unroll):
                head = group * reps + at[i]
                scores = scaled_scores(keys, head)
                if keep:
                    sbuf[slot(group, block, at[i])] = scores
                top = jnp.full((1, text), FLOOR, F32) if first else mst[pl.ds(head, 1), :]
                for t, part in enumerate(tiles_of(scores)):
                    top = jnp.maximum(top, jnp.max(part, axis=0, keepdims=True) - hide[t])
                kept.append(scores)
                tops.append(top)
            for i in range(unroll):
                head = group * reps + at[i]
                weights = jnp.concatenate(
                    [jnp.exp2(part - (tops[i] + hide[t])) for t, part in enumerate(tiles_of(kept[i]))],
                    axis=0,
                ).astype(BF16)
                both = jnp.dot(values_t, weights, preferred_element_type=F32)
                numer, total = both[:HD], both[HD : HD + 1]
                if not first:
                    shrink = jnp.exp2(mst[pl.ds(head, 1), :] - tops[i])
                    total = total + tst[pl.ds(head, 1), :] * shrink
                    numer = numer + numt[head] * shrink
                totals.append(total)
                outs.append(numer)
            for i in range(unroll):
                head = group * reps + at[i]
                mst[pl.ds(head, 1), :] = tops[i]
                tst[pl.ds(head, 1), :] = totals[i]
                numt[head] = outs[i]
            return 0

        lax.fori_loop(0, reps // unroll, body, 0)

    def group_rows(group):
        return pl.ds(group * reps, reps)

    def stats_copies(group):
        return [
            remote(
                stbuf.at[group, img], stbuf.at[group, img], st_ss.at[group, step - 1],
                st_rs.at[group, step - 1], "img", lax.rem(img + step, ni),
            )
            for step in range(1, ni)
        ]

    def stats_start(group):
        def deltas(at, _):
            head = group * reps + at
            stbuf[group, img, 2, pl.ds(at, 1), :] = jnp.sum(
                gt[head].astype(F32) * numt[head], axis=0, keepdims=True
            )
            return 0

        lax.fori_loop(0, reps, deltas, 0)
        stbuf[group, img, 0] = mst[group_rows(group), :]
        stbuf[group, img, 1] = tst[group_rows(group), :]
        for copy in stats_copies(group):
            copy.start()

    def stats_finish(group):
        for copy in stats_copies(group):
            copy.wait_recv()
        top = stbuf[group, 0, 0]
        for i in range(1, ni):
            top = jnp.maximum(top, stbuf[group, i, 0])
        total = jnp.zeros_like(top)
        delta = jnp.zeros_like(top)
        for i in range(ni):
            factor = jnp.exp2(stbuf[group, i, 0] - top)
            total = total + factor * stbuf[group, i, 1]
            delta = delta + factor * stbuf[group, i, 2]
        lse[group_rows(group), :] = top + jnp.log(total) * LOG2E
        dlt[group_rows(group), :] = delta / total
        cown[group_rows(group), :] = jnp.exp2(stbuf[group, img, 0] - top) / total

    def goal(step):
        return pick(txt, [depart[z][step] for z in range(nt)])

    def grad_copy(group, step, part):
        block = goal(step)
        up = block > txt
        target = jnp.where(up, txt + 1, txt - 1)
        back = jnp.where(up, txt - 1, txt + 1)
        lands = jnp.where(jnp.logical_and(target == block, jnp.logical_not(up)), nt, block)
        copy = remote(
            gsend.at[group, step, part], grecv.at[group, lands, part],
            g_ss.at[group, step, part], g_rs.at[group, lands, part], "txt", target,
        )
        relayed = jnp.logical_and(back >= 0, back < nt)
        return copy, relayed, block

    def grad_wait(group, place, part):
        remote(
            gsend.at[group, 0, part], grecv.at[group, place, part],
            g_ss.at[group, 0, part], g_rs.at[group, place, part], "txt", txt,
        ).wait_recv()

    def backward(group, step):
        block = goal(step)

        def body(turn, _):
            at = [turn * unroll + i for i in range(unroll)]
            keys, values = kvbuf[group, block, 0], kvbuf[group, block, 1]
            hide = [big[pl.ds(block * block_tiles + t, 1), :] for t in range(block_tiles)]
            probs_all, grads_all = [], []
            for i in range(unroll):
                head = group * reps + at[i]
                grad_probs = jnp.dot(values, gt[head], preferred_element_type=F32)
                if keep:
                    scores = sbuf[slot(group, block, at[i])]
                else:
                    scores = scaled_scores(keys, head)
                base = lse[pl.ds(head, 1), :]
                probs = jnp.concatenate(
                    [jnp.exp2(part - (base + hide[t])) for t, part in enumerate(tiles_of(scores))],
                    axis=0,
                )
                grads_all.append((probs * (grad_probs - dlt[pl.ds(head, 1), :])).astype(BF16))
                probs_all.append(probs.astype(BF16))
            picked = [group * reps + a for a in at]
            queries = jnp.concatenate([qt[head] for head in picked], axis=1)
            grads = jnp.concatenate([gt[head] for head in picked], axis=1)
            gpart[step, 0] = gpart[step, 0] + lax.dot_general(
                queries, jnp.concatenate(grads_all, axis=1), NT, preferred_element_type=F32
            )
            gpart[step, 1] = gpart[step, 1] + lax.dot_general(
                grads, jnp.concatenate(probs_all, axis=1), NT, preferred_element_type=F32
            )
            return 0

        gpart[step] = jnp.zeros_like(gpart[step])
        lax.fori_loop(0, reps // unroll, body, 0)

    def grown(step, part):
        value = gpart[step, part]
        return value * scale if part == 0 else value

    def leave(group, step):
        for part in range(2):
            copy, relayed, _ = grad_copy(group, step, part)

            def go(copy=copy, part=part):
                gsend[group, step, part] = grown(step, part).astype(BF16)
                copy.start()

            pl.when(jnp.logical_not(relayed))(go)

    def pass_on(group, step):
        for part in range(2):
            copy, relayed, block = grad_copy(group, step, part)

            def go(copy=copy, part=part, block=block):
                grad_wait(group, block, part)
                gsend[group, step, part] = (
                    grown(step, part) + grecv[group, block, part].astype(F32)
                ).astype(BF16)
                copy.start()

            pl.when(relayed)(go)

    def h_copy(step, group, part):
        mine = hall.at[hd, group, part]
        at = (step - 1, group, part)
        return remote(mine, mine, h_ss.at[at], h_rs.at[at], "head", other(step))

    def own_grad(group):
        for part in range(2):
            gpart[nt - 1, part] = grown(nt - 1, part)
            for there, place in ((txt > 0, txt), (txt < nt - 1, jnp.int32(nt))):

                def add(place=place, part=part):
                    grad_wait(group, place, part)
                    gpart[nt - 1, part] = gpart[nt - 1, part] + grecv[group, place, part].astype(F32)

                pl.when(there)(add)
            hall[hd, group, part] = gpart[nt - 1, part].T.astype(BF16)
            for step in range(1, nh):
                h_copy(step, group, part).start()

    lower = lax.rem(img, 2)
    mate = img + 1 - 2 * lower
    mine_rows = pl.ds(pl.multiple_of(lower * half, half), half)
    mate_rows = pl.ds(pl.multiple_of((1 - lower) * half, half), half)

    def flip(bit):
        return img + (1 << bit) - (2 << bit) * lax.rem(img // (1 << bit), 2)

    def out_cols(group):
        return pl.ds(group * gcols, gcols)

    def pair_copy(group):
        return remote(
            qraw.at[mate_rows, out_cols(group)], ocr.at[group], oc_ss.at[group], oc_rs.at[group],
            "img", mate,
        )

    def cross_copy(group, bit):
        at = (group, bit - 1)
        return remote(xs.at[at], xr.at[at], ox_ss.at[at], ox_rs.at[at], "img", flip(bit))

    def share_copy(group):
        there = graw.at[mine_rows, out_cols(group)]
        return remote(there, there, oa_ss.at[group], oa_rs.at[group], "img", mate)

    def outputs(group):
        def body(at, _):
            head = group * reps + at
            cols = pl.ds(pl.multiple_of(head * HD, HD), HD)
            qraw[:, cols] = (numt[head] * cown[pl.ds(head, 1), :]).T.astype(BF16)
            return 0

        lax.fori_loop(0, reps, body, 0)
        pair_copy(group).start()

    def cross(group):
        pair_copy(group).wait_recv()
        total = qraw[mine_rows, out_cols(group)].astype(F32) + ocr[group].astype(F32)
        if bits > 1:
            xs[group, 0] = total.astype(BF16)
            cross_copy(group, 1).start()
        else:
            graw[mine_rows, out_cols(group)] = total.astype(BF16)
            share_copy(group).start()

    def share(group):
        for bit in range(1, bits):
            cross_copy(group, bit).wait_recv()
            total = (xs[group, bit - 1].astype(F32) + xr[group, bit - 1].astype(F32)).astype(BF16)
            if bit < bits - 1:
                xs[group, bit] = total
                cross_copy(group, bit + 1).start()
            else:
                graw[mine_rows, out_cols(group)] = total
                share_copy(group).start()

    def finish_output(group):
        share_copy(group).wait_recv()
        attn[:, out_cols(group)] = graw[:, out_cols(group)]

    per = math.gcd(width // text, 3)
    chunk = per * text

    def features(pairs, first, last):
        def body(at, _):
            span = pl.ds(pl.multiple_of(at * chunk, chunk), chunk)
            left = jnp.concatenate([hall[o, group, p] for o, group in pairs for p in range(2)], axis=1)
            right = jnp.concatenate(
                [w[span, cols_of(o, group)] for o, group in pairs for w in (kw, vw)], axis=1
            )
            value = lax.dot_general(left, right, NT, preferred_element_type=F32)
            for j in range(per):
                piece = value[:, j * text : (j + 1) * text]
                if not first:
                    piece = piece + sbuf[at * per + j]
                if last:
                    start = pl.multiple_of(at * chunk + j * text, text)
                    dfeats[:, pl.ds(start, text)] = piece.astype(BF16)
                else:
                    sbuf[at * per + j] = piece
            return 0

        lax.fori_loop(0, width // chunk, body, 0)

    def h_wait(group):
        for step in range(1, nh):
            for part in range(2):
                h_copy(step, group, part).wait_recv()

    for part in range(2):
        own_sum(0, part)

        def go(part=part, side=0):
            kv_copy(0, part, side).start()

        for side in range(2):
            pl.when(has_side[side])(functools.partial(go, part, side))
    q_load.wait()
    g_load.wait()
    turn_over(0)
    forward(0, txt, True)
    for part in range(2):
        own_sum(1, part)
    send_own(1, 0)
    for step in range(1, nt):
        receive(0, step)
        send_own(1, step)
        forward(0, arrival(0, step)[0], False)
        if step == 1:
            turn_over(1)
    stats_start(0)
    forward(1, txt, True)
    receive(1, 1)
    stats_finish(0)
    for step in range(nt - 1):
        backward(0, step)
        leave(0, step)
        if step + 2 < nt:
            receive(1, step + 2)
        if step >= 1:
            pass_on(0, step - 1)
    for step in range(1, nt):
        forward(1, arrival(1, step)[0], False)
    stats_start(1)
    pass_on(0, nt - 2)
    backward(0, nt - 1)
    outputs(0)
    stats_finish(1)
    for step in range(nt - 1):
        if step == 1:
            own_grad(0)
            outputs(1)
            cross(0)
        backward(1, step)
        leave(1, step)
        if step >= 1:
            pass_on(1, step - 1)
    backward(1, nt - 1)
    pass_on(1, nt - 2)
    cross(1)
    share(0)
    h_wait(0)
    owners = [hd] + [other(step) for step in range(1, nh)]
    features([(o, 0) for o in owners], True, False)
    own_grad(1)
    features([(hd, 1)], False, False)
    share(1)
    finish_output(0)
    finish_output(1)
    h_wait(1)
    features([(o, 1) for o in owners[1:]], False, True)

    for copy in p_copies.values():
        copy.wait_send()
    for group in range(groups):
        for side in range(2):

            def own_sent(group=group, side=side):
                for part in range(2):
                    kv_copy(group, part, side).wait_send()

            pl.when(has_side[side])(own_sent)
        for step in range(1, nt):
            _, valid, copies = arrival(group, step)

            def passed(copies=copies):
                for copy in copies:
                    copy.wait_send()

            pl.when(valid)(passed)
        for copy in stats_copies(group):
            copy.wait_send()
        for step in range(nt - 1):
            for part in range(2):
                grad_copy(group, step, part)[0].wait_send()
        pair_copy(group).wait_send()
        for bit in range(1, bits):
            cross_copy(group, bit).wait_send()
        share_copy(group).wait_send()
        for step in range(1, nh):
            for part in range(2):
                h_copy(step, group, part).wait_send()


def shards(sizes, image_feats, key_weight, value_weight, queries, grad_out, tile_image, text_sees):
    ni, nh, nt = sizes
    rows, feat_width = image_feats.shape
    text, width = queries.shape
    heads = width // HD
    own_cols = key_weight.shape[1] // nh
    groups = own_cols // HD
    reps = heads // groups
    half = text // 2
    gcols = reps * HD
    tiles = nt * rows // TILE
    crosses = max(ni.bit_length() - 2, 1)
    slots = feat_width // text
    keep = nt * heads * rows * text * 4 <= VMEM_BUDGET // 3
    if keep:
        slots = max(slots, nt * heads)
    dma = pltpu.SemaphoreType.DMA
    hbm = pl.BlockSpec(memory_space=pl.ANY)
    vmem = pl.BlockSpec(memory_space=pltpu.VMEM)
    smem = pl.BlockSpec(memory_space=pltpu.SMEM)
    attn, grad_feats = pl.pallas_call(
        functools.partial(kernel, sizes, keep),
        out_shape=(
            pltpu.VMEM((text, width), BF16),
            pltpu.VMEM(image_feats.shape, BF16),
        ),
        in_specs=[hbm] * 5 + [smem] * 2,
        out_specs=(vmem, vmem),
        scratch_shapes=[
            pltpu.VMEM(image_feats.shape, BF16),
            pltpu.VMEM(key_weight.shape, BF16),
            pltpu.VMEM(value_weight.shape, BF16),
            pltpu.VMEM((text, width), BF16),
            pltpu.VMEM((text, width), BF16),
            pltpu.VMEM((heads, HD, text), BF16),
            pltpu.VMEM((heads, HD, text), BF16),
            pltpu.VMEM((tiles, text), F32),
            pltpu.VMEM((nh - 1, groups, 2, rows, HD), BF16),
            pltpu.VMEM((nh - 1, groups, 2, rows, HD), BF16),
            pltpu.VMEM((groups, rows, 2 * HD), F32),
            pltpu.VMEM((groups, nt, 2, rows, HD), BF16),
            pltpu.VMEM((HD + ONES, rows), BF16),
            pltpu.VMEM((slots, rows, text), F32),
            pltpu.VMEM((heads, HD, text), F32),
            pltpu.VMEM((heads, text), F32),
            pltpu.VMEM((heads, text), F32),
            pltpu.VMEM((groups, ni, 3, reps, text), F32),
            pltpu.VMEM((heads, text), F32),
            pltpu.VMEM((heads, text), F32),
            pltpu.VMEM((heads, text), F32),
            pltpu.VMEM((groups, nt - 1, 2, HD, rows), BF16),
            pltpu.VMEM((groups, nt + 1, 2, HD, rows), BF16),
            pltpu.VMEM((nt, 2, HD, rows), F32),
            pltpu.VMEM((nh, groups, 2, rows, HD), BF16),
            pltpu.VMEM((groups, half, gcols), BF16),
            pltpu.VMEM((groups, crosses, half, gcols), BF16),
            pltpu.VMEM((groups, crosses, half, gcols), BF16),
            dma((3,)), dma((nh, groups, 2)),
            dma((nh - 1, groups, 2)), dma((nh - 1, groups, 2)),
            dma((groups, 2, 2)), dma((groups, nt, 2)), dma((groups, nt, 2)),
            dma((groups, ni - 1)), dma((groups, ni - 1)),
            dma((groups,)), dma((groups,)),
            dma((groups, crosses)), dma((groups, crosses)),
            dma((groups,)), dma((groups,)),
            dma((groups, nt - 1, 2)), dma((groups, nt + 1, 2)),
            dma((nh - 1, groups, 2)), dma((nh - 1, groups, 2)),
        ],
        compiler_params=pltpu.CompilerParams(
            collective_id=0, has_side_effects=True, vmem_limit_bytes=VMEM_BUDGET
        ),
    )(image_feats, key_weight, value_weight, queries, grad_out, tile_image, text_sees)
    return (attn, grad_feats)


def solution(mesh):
    sizes = (mesh.shape["img"], mesh.shape["head"], mesh.shape["txt"])
    placed = (
        P(("img", "txt"), "head"),
        P("head", None),
        P("head", None),
        P("txt", "head"),
        P("txt", "head"),
        P("img"),
        P(),
    )
    return jax.shard_map(
        functools.partial(shards, sizes),
        mesh=mesh,
        in_specs=placed,
        out_specs=(P("txt", "head"), P(("img", "txt"), "head")),
        check_vma=False,
    )
```

```python
import functools
import math

import jax
import jax.numpy as jnp
from jax import lax
from jax.experimental import pallas as pl
from jax.experimental.pallas import tpu as pltpu
from jax.sharding import PartitionSpec as P

HD = 128
TILE = 128
TBLK = 128
MESH = pl.DeviceIdType.MESH
UNROLL = 4
LOG2E = 1.4426950408889634
NT = (((1,), (1,)), ((), ()))
F32 = jnp.float32
BF16 = jnp.bfloat16
HIDE = 2e30
FLOOR = -1e30
ONES = 16
VMEM_BUDGET = 58 * 1024 * 1024


def pick(index, table):
    value = jnp.int32(table[0])
    for at in range(1, len(table)):
        value = jnp.where(index == at, jnp.int32(table[at]), value)
    return value


def arrival_order(count):
    return [
        sorted((b for b in range(count) if b != z), key=lambda b: (abs(b - z), b))
        for z in range(count)
    ]


def departure_order(count):
    orders = []
    for z in range(count):
        above, below = list(range(count - 1, z, -1)), list(range(z))
        orders.append((above + below if 2 * z < count else below + above[::-1]) + [z])
    return orders


def kernel(
    sizes, keep,
    feats_hbm, kw_hbm, vw_hbm, q_hbm, g_hbm, tile_image, text_sees,
    attn, dfeats,
    feats, kw, vw, qraw, graw, qt, gt, big, psend, precv, pacc, kvbuf, vtb, sbuf, numt, mst, tst,
    stbuf, lse, dlt, cown, gsend, grecv, gpart, hall, ocr, xs, xr,
    l_s, w_s, p_ss, p_rs, kv_ss, kv_fs, kv_rs, st_ss, st_rs, oc_ss, oc_rs, ox_ss, ox_rs,
    oa_ss, oa_rs, g_ss, g_rs, h_ss, h_rs,
):
    ni, nh, nt = sizes
    img, hd, txt = lax.axis_index("img"), lax.axis_index("head"), lax.axis_index("txt")
    rows, width = feats.shape
    groups = kvbuf.shape[0]
    own_cols = groups * HD
    text = qraw.shape[0]
    heads = qraw.shape[1] // HD
    reps = heads // groups
    block_tiles = rows // TILE
    scale = 1.0 / math.sqrt(HD)
    unroll = math.gcd(UNROLL, reps)
    half = text // 2
    gcols = reps * HD
    bits = ni.bit_length() - 1
    arrive, depart = arrival_order(nt), departure_order(nt)
    relay = nt == 4
    inner = jnp.logical_or(txt == 1, txt == 2)
    outer = jnp.logical_not(inner)

    def cols_of(owner, group):
        return pl.ds(pl.multiple_of(owner * own_cols + group * HD, HD), HD)

    def other(step):
        return lax.rem(hd + step, nh)

    loads = [pltpu.make_async_copy(feats_hbm, feats, l_s.at[0])]
    weight_loads = {}
    for step in list(range(1, nh)) + [0]:
        for group in range(groups):
            cols = cols_of(other(step), group)
            pair = [
                pltpu.make_async_copy(src.at[:, cols], dst.at[:, cols], w_s.at[step, group, part])
                for part, (src, dst) in enumerate(((kw_hbm, kw), (vw_hbm, vw)))
            ]
            weight_loads[step, group] = pair
            loads += pair
    q_load = pltpu.make_async_copy(q_hbm, qraw, l_s.at[1])
    g_load = pltpu.make_async_copy(g_hbm, graw, l_s.at[2])
    loads += [q_load, g_load]
    for copy in loads:
        copy.start()

    barrier = pltpu.get_barrier_semaphore()
    for step in range(1, nh):
        pl.semaphore_signal(barrier, inc=1, device_id={"head": other(step)}, device_id_type=MESH)
    for step in range(1, nt):
        pl.semaphore_signal(barrier, inc=1, device_id={"txt": lax.rem(txt + step, nt)}, device_id_type=MESH)
    for step in range(1, ni):
        pl.semaphore_signal(barrier, inc=1, device_id={"img": lax.rem(img + step, ni)}, device_id_type=MESH)

    def remote(src, dst, ss, rs, axis, index):
        return pltpu.make_async_remote_copy(
            src_ref=src, dst_ref=dst, send_sem=ss, recv_sem=rs,
            device_id={axis: index}, device_id_type=MESH,
        )

    first_block = txt * (text // TBLK)
    for tile in range(big.shape[0]):
        image = tile_image[tile]
        parts = [
            jnp.full((1, TBLK), text_sees[first_block + at, image].astype(F32))
            for at in range(text // TBLK)
        ]
        seen = jnp.concatenate(parts, axis=1)
        big[pl.ds(tile, 1), :] = jnp.where(seen > 0.5, 0.0, HIDE)
    vtb[pl.ds(HD, ONES), :] = jnp.ones((ONES, rows), BF16)

    def project(step, group):
        for copy in weight_loads[step, group]:
            copy.wait()
        cols = cols_of(other(step), group)
        weights = jnp.concatenate([kw[:, cols], vw[:, cols]], axis=1)
        return jnp.dot(feats[...], weights, preferred_element_type=F32)

    loads[0].wait()
    p_copies = {}
    for step in range(1, nh):
        for group in range(groups):
            value = project(step, group).astype(BF16)
            if step == 1 and group == 0:
                pl.semaphore_wait(barrier, nh - 1 + nt - 1 + ni - 1)
            for part in range(2):
                psend[step - 1, group, part] = value[:, part * HD : (part + 1) * HD]
                at = (step - 1, group, part)
                copy = remote(
                    psend.at[at], precv.at[at], p_ss.at[at], p_rs.at[at], "head", other(step)
                )
                copy.start()
                p_copies[at] = copy
    for group in range(groups):
        pacc[group] = project(0, group)

    def own_sum(group, part):
        total = pacc[group, :, part * HD : (part + 1) * HD]
        for step in range(1, nh):
            p_copies[step - 1, group, part].wait_recv()
            total = total + precv[step - 1, group, part].astype(F32)
        kvbuf[group, txt, part] = total.astype(BF16)

    near = [[b for b in arrive[z] if not (relay and abs(b - z) == 3)] for z in range(nt)]
    most = max(len(places) for places in near)

    def own_copies(group, part):
        mine = kvbuf.at[group, txt, part]
        for at in range(most):
            there = pick(txt, [places[at] if at < len(places) else -1 for places in near])
            yield there >= 0, remote(
                mine, mine, kv_ss.at[group, part, at], kv_rs.at[group, txt, part], "txt", there
            )

    def send_own(group, parts):
        for part in parts:
            for valid, copy in own_copies(group, part):
                pl.when(valid)(copy.start)

    def block_at(step):
        return pick(txt, [arrive[z][step - 1] for z in range(nt)])

    def relay_copy(group, part):
        there = kvbuf.at[group, block_at(nt - 1), part]
        return remote(
            there, there, kv_fs.at[group, part], kv_rs.at[group, block_at(nt - 1), part],
            "txt", jnp.where(txt == 1, 0, nt - 1),
        )

    def receive(group, step):
        block = block_at(step)
        for part in range(2):
            there = kvbuf.at[group, block, part]
            remote(
                there, there, kv_ss.at[group, part, 0], kv_rs.at[group, block, part], "txt", txt
            ).wait_recv()

    def pass_block(group, then=None):
        def go():
            for part in range(2):
                relay_copy(group, part).wait_recv()
                relay_copy(group, part).start()
            if then is not None:
                then()

        if relay:
            pl.when(inner)(go)
        elif then is not None:
            then()

    def receive_last(group):
        if relay:
            pl.when(outer)(lambda: receive(group, nt - 1))
        else:
            receive(group, nt - 1)

    def turn_over(group):
        def body(at, _):
            head = group * reps + at
            cols = pl.ds(pl.multiple_of(head * HD, HD), HD)
            qt[head] = qraw[:, cols].astype(F32).T.astype(BF16)
            gt[head] = graw[:, cols].astype(F32).T.astype(BF16)
            return 0

        lax.fori_loop(0, reps, body, 0)

    def scaled_scores(keys, head):
        return jnp.dot(keys, qt[head], preferred_element_type=F32) * (scale * LOG2E)

    def tiles_of(array):
        return [array[t * TILE : (t + 1) * TILE] for t in range(block_tiles)]

    def slot(group, block, at):
        return (group * nt + block) * reps + at

    def forward(group, block, first):
        vtb[pl.ds(0, HD), :] = kvbuf[group, block, 1].astype(F32).T.astype(BF16)

        def body(turn, _):
            at = [turn * unroll + i for i in range(unroll)]
            keys, values_t = kvbuf[group, block, 0], vtb[...]
            hide = [big[pl.ds(block * block_tiles + t, 1), :] for t in range(block_tiles)]
            kept, tops, totals, outs = [], [], [], []
            for i in range(unroll):
                head = group * reps + at[i]
                scores = scaled_scores(keys, head)
                if keep:
                    sbuf[slot(group, block, at[i])] = scores
                top = jnp.full((1, text), FLOOR, F32) if first else mst[pl.ds(head, 1), :]
                for t, part in enumerate(tiles_of(scores)):
                    top = jnp.maximum(top, jnp.max(part, axis=0, keepdims=True) - hide[t])
                kept.append(scores)
                tops.append(top)
            for i in range(unroll):
                head = group * reps + at[i]
                weights = jnp.concatenate(
                    [jnp.exp2(part - (tops[i] + hide[t])) for t, part in enumerate(tiles_of(kept[i]))],
                    axis=0,
                ).astype(BF16)
                both = jnp.dot(values_t, weights, preferred_element_type=F32)
                numer, total = both[:HD], both[HD : HD + 1]
                if not first:
                    shrink = jnp.exp2(mst[pl.ds(head, 1), :] - tops[i])
                    total = total + tst[pl.ds(head, 1), :] * shrink
                    numer = numer + numt[head] * shrink
                totals.append(total)
                outs.append(numer)
            for i in range(unroll):
                head = group * reps + at[i]
                mst[pl.ds(head, 1), :] = tops[i]
                tst[pl.ds(head, 1), :] = totals[i]
                numt[head] = outs[i]
            return 0

        lax.fori_loop(0, reps // unroll, body, 0)

    def group_rows(group):
        return pl.ds(group * reps, reps)

    def stats_copies(group):
        return [
            remote(
                stbuf.at[group, img], stbuf.at[group, img], st_ss.at[group, step - 1],
                st_rs.at[group, step - 1], "img", lax.rem(img + step, ni),
            )
            for step in range(1, ni)
        ]

    def stats_start(group):
        def deltas(at, _):
            head = group * reps + at
            stbuf[group, img, 2, pl.ds(at, 1), :] = jnp.sum(
                gt[head].astype(F32) * numt[head], axis=0, keepdims=True
            )
            return 0

        lax.fori_loop(0, reps, deltas, 0)
        stbuf[group, img, 0] = mst[group_rows(group), :]
        stbuf[group, img, 1] = tst[group_rows(group), :]
        for copy in stats_copies(group):
            copy.start()

    def stats_finish(group):
        for copy in stats_copies(group):
            copy.wait_recv()
        top = stbuf[group, 0, 0]
        for i in range(1, ni):
            top = jnp.maximum(top, stbuf[group, i, 0])
        total = jnp.zeros_like(top)
        delta = jnp.zeros_like(top)
        for i in range(ni):
            factor = jnp.exp2(stbuf[group, i, 0] - top)
            total = total + factor * stbuf[group, i, 1]
            delta = delta + factor * stbuf[group, i, 2]
        lse[group_rows(group), :] = top + jnp.log(total) * LOG2E
        dlt[group_rows(group), :] = delta / total
        cown[group_rows(group), :] = jnp.exp2(stbuf[group, img, 0] - top) / total

    def goal(step):
        return pick(txt, [depart[z][step] for z in range(nt)])

    def grad_copy(group, step, part):
        target, lands = goal(step), txt
        if relay and step == 0:
            target = pick(txt, [1, nt - 1, 0, 2])
            lands = jnp.where(outer, nt, txt)
        return remote(
            gsend.at[group, step, part], grecv.at[group, lands, part],
            g_ss.at[group, step, part], g_rs.at[group, lands, part], "txt", target,
        )

    def grad_wait(group, place, part):
        remote(
            gsend.at[group, 0, part], grecv.at[group, place, part],
            g_ss.at[group, 0, part], g_rs.at[group, place, part], "txt", txt,
        ).wait_recv()

    def backward(group, step):
        block = goal(step)

        def body(turn, _):
            at = [turn * unroll + i for i in range(unroll)]
            keys, values = kvbuf[group, block, 0], kvbuf[group, block, 1]
            hide = [big[pl.ds(block * block_tiles + t, 1), :] for t in range(block_tiles)]
            probs_all, grads_all = [], []
            for i in range(unroll):
                head = group * reps + at[i]
                grad_probs = jnp.dot(values, gt[head], preferred_element_type=F32)
                if keep:
                    scores = sbuf[slot(group, block, at[i])]
                else:
                    scores = scaled_scores(keys, head)
                base = lse[pl.ds(head, 1), :]
                probs = jnp.concatenate(
                    [jnp.exp2(part - (base + hide[t])) for t, part in enumerate(tiles_of(scores))],
                    axis=0,
                )
                grads_all.append((probs * (grad_probs - dlt[pl.ds(head, 1), :])).astype(BF16))
                probs_all.append(probs.astype(BF16))
            picked = [group * reps + a for a in at]
            queries = jnp.concatenate([qt[head] for head in picked], axis=1)
            grads = jnp.concatenate([gt[head] for head in picked], axis=1)
            gpart[step, 0] = gpart[step, 0] + lax.dot_general(
                queries, jnp.concatenate(grads_all, axis=1), NT, preferred_element_type=F32
            )
            gpart[step, 1] = gpart[step, 1] + lax.dot_general(
                grads, jnp.concatenate(probs_all, axis=1), NT, preferred_element_type=F32
            )
            return 0

        gpart[step] = jnp.zeros_like(gpart[step])
        lax.fori_loop(0, reps // unroll, body, 0)

    def grown(step, part):
        value = gpart[step, part]
        return value * scale if part == 0 else value

    def leave(group, step):
        def go():
            for part in range(2):
                gsend[group, step, part] = grown(step, part).astype(BF16)
                grad_copy(group, step, part).start()

        if relay and step == 0:
            pl.when(outer)(go)
        else:
            go()

    def pass_on(group):
        def go():
            for part in range(2):
                grad_wait(group, nt, part)
                gsend[group, 0, part] = (
                    grown(0, part) + grecv[group, nt, part].astype(F32)
                ).astype(BF16)
                grad_copy(group, 0, part).start()

        if relay:
            pl.when(inner)(go)

    def h_copy(step, group, part):
        mine = hall.at[hd, group, part]
        at = (step - 1, group, part)
        return remote(mine, mine, h_ss.at[at], h_rs.at[at], "head", other(step))

    def own_grad(group):
        for part in range(2):
            gpart[nt - 1, part] = grown(nt - 1, part)

            def add(step, part=part):
                place = block_at(step)
                grad_wait(group, place, part)
                gpart[nt - 1, part] = gpart[nt - 1, part] + grecv[group, place, part].astype(F32)

            for step in range(1, nt):
                if relay and step == nt - 1:
                    pl.when(inner)(functools.partial(add, step))
                else:
                    add(step)
            hall[hd, group, part] = gpart[nt - 1, part].T.astype(BF16)
            for step in range(1, nh):
                h_copy(step, group, part).start()

    lower = lax.rem(img, 2)
    mate = img + 1 - 2 * lower
    mine_rows = pl.ds(pl.multiple_of(lower * half, half), half)
    mate_rows = pl.ds(pl.multiple_of((1 - lower) * half, half), half)

    def flip(bit):
        return img + (1 << bit) - (2 << bit) * lax.rem(img // (1 << bit), 2)

    def out_cols(group):
        return pl.ds(group * gcols, gcols)

    def pair_copy(group):
        return remote(
            qraw.at[mate_rows, out_cols(group)], ocr.at[group], oc_ss.at[group], oc_rs.at[group],
            "img", mate,
        )

    def cross_copy(group, bit):
        at = (group, bit - 1)
        return remote(xs.at[at], xr.at[at], ox_ss.at[at], ox_rs.at[at], "img", flip(bit))

    def share_copy(group):
        there = graw.at[mine_rows, out_cols(group)]
        return remote(there, there, oa_ss.at[group], oa_rs.at[group], "img", mate)

    def outputs(group):
        def body(at, _):
            head = group * reps + at
            cols = pl.ds(pl.multiple_of(head * HD, HD), HD)
            qraw[:, cols] = (numt[head] * cown[pl.ds(head, 1), :]).T.astype(BF16)
            return 0

        lax.fori_loop(0, reps, body, 0)
        pair_copy(group).start()

    def cross(group):
        pair_copy(group).wait_recv()
        total = qraw[mine_rows, out_cols(group)].astype(F32) + ocr[group].astype(F32)
        if bits > 1:
            xs[group, 0] = total.astype(BF16)
            cross_copy(group, 1).start()
        else:
            graw[mine_rows, out_cols(group)] = total.astype(BF16)
            share_copy(group).start()

    def share(group):
        for bit in range(1, bits):
            cross_copy(group, bit).wait_recv()
            total = (xs[group, bit - 1].astype(F32) + xr[group, bit - 1].astype(F32)).astype(BF16)
            if bit < bits - 1:
                xs[group, bit] = total
                cross_copy(group, bit + 1).start()
            else:
                graw[mine_rows, out_cols(group)] = total
                share_copy(group).start()

    def finish_output(group):
        share_copy(group).wait_recv()
        attn[:, out_cols(group)] = graw[:, out_cols(group)]

    per = math.gcd(width // text, 3)
    chunk = per * text

    def features(pairs, first, last):
        def body(at, _):
            span = pl.ds(pl.multiple_of(at * chunk, chunk), chunk)
            left = jnp.concatenate([hall[o, group, p] for o, group in pairs for p in range(2)], axis=1)
            right = jnp.concatenate(
                [w[span, cols_of(o, group)] for o, group in pairs for w in (kw, vw)], axis=1
            )
            value = lax.dot_general(left, right, NT, preferred_element_type=F32)
            for j in range(per):
                piece = value[:, j * text : (j + 1) * text]
                if not first:
                    piece = piece + sbuf[at * per + j]
                if last:
                    start = pl.multiple_of(at * chunk + j * text, text)
                    dfeats[:, pl.ds(start, text)] = piece.astype(BF16)
                else:
                    sbuf[at * per + j] = piece
            return 0

        lax.fori_loop(0, width // chunk, body, 0)

    def h_wait(group):
        for step in range(1, nh):
            for part in range(2):
                h_copy(step, group, part).wait_recv()

    q_load.wait()
    g_load.wait()
    turn_over(0)
    for part in range(2):
        own_sum(0, part)
        send_own(0, [part])
    forward(0, txt, True)
    for part in range(2):
        own_sum(1, part)
    if relay:
        pl.when(outer)(lambda: send_own(1, range(2)))
    for step in range(1, nt - 1):
        receive(0, step)
        forward(0, block_at(step), False)
        if step == 1:
            turn_over(1)
    pass_block(0, lambda: send_own(1, range(2)))
    receive_last(0)
    forward(0, block_at(nt - 1), False)
    stats_start(0)
    forward(1, txt, True)
    receive(1, 1)
    forward(1, block_at(1), False)
    stats_finish(0)
    backward(0, 0)
    leave(0, 0)
    backward(0, 1)
    leave(0, 1)
    pass_block(1)
    pass_on(0)
    for step in range(2, nt - 1):
        receive(1, step)
        forward(1, block_at(step), False)
        backward(0, step)
        leave(0, step)
    backward(0, nt - 1)
    outputs(0)
    receive_last(1)
    forward(1, block_at(nt - 1), False)
    stats_start(1)
    own_grad(0)
    cross(0)
    stats_finish(1)
    for step in range(nt - 1):
        backward(1, step)
        leave(1, step)
        if step == 1:
            pass_on(1)
    outputs(1)
    backward(1, nt - 1)
    share(0)
    h_wait(0)
    owners = [hd] + [other(step) for step in range(1, nh)]
    features([(o, 0) for o in owners], True, False)
    cross(1)
    own_grad(1)
    features([(hd, 1)], False, False)
    share(1)
    finish_output(0)
    finish_output(1)
    h_wait(1)
    features([(o, 1) for o in owners[1:]], False, True)

    for copy in p_copies.values():
        copy.wait_send()
    for group in range(groups):
        for part in range(2):
            for valid, copy in own_copies(group, part):
                pl.when(valid)(copy.wait_send)
            if relay:
                pl.when(inner)(relay_copy(group, part).wait_send)
            for step in range(nt - 1):
                grad_copy(group, step, part).wait_send()
        for copy in stats_copies(group):
            copy.wait_send()
        pair_copy(group).wait_send()
        for bit in range(1, bits):
            cross_copy(group, bit).wait_send()
        share_copy(group).wait_send()
        for step in range(1, nh):
            for part in range(2):
                h_copy(step, group, part).wait_send()


def shards(sizes, image_feats, key_weight, value_weight, queries, grad_out, tile_image, text_sees):
    ni, nh, nt = sizes
    rows, feat_width = image_feats.shape
    text, width = queries.shape
    heads = width // HD
    own_cols = key_weight.shape[1] // nh
    groups = own_cols // HD
    reps = heads // groups
    half = text // 2
    gcols = reps * HD
    tiles = nt * rows // TILE
    crosses = max(ni.bit_length() - 2, 1)
    slots = feat_width // text
    keep = nt * heads * rows * text * 4 <= VMEM_BUDGET // 3
    if keep:
        slots = max(slots, nt * heads)
    dma = pltpu.SemaphoreType.DMA
    hbm = pl.BlockSpec(memory_space=pl.ANY)
    vmem = pl.BlockSpec(memory_space=pltpu.VMEM)
    smem = pl.BlockSpec(memory_space=pltpu.SMEM)
    attn, grad_feats = pl.pallas_call(
        functools.partial(kernel, sizes, keep),
        out_shape=(
            pltpu.VMEM((text, width), BF16),
            pltpu.VMEM(image_feats.shape, BF16),
        ),
        in_specs=[hbm] * 5 + [smem] * 2,
        out_specs=(vmem, vmem),
        scratch_shapes=[
            pltpu.VMEM(image_feats.shape, BF16),
            pltpu.VMEM(key_weight.shape, BF16),
            pltpu.VMEM(value_weight.shape, BF16),
            pltpu.VMEM((text, width), BF16),
            pltpu.VMEM((text, width), BF16),
            pltpu.VMEM((heads, HD, text), BF16),
            pltpu.VMEM((heads, HD, text), BF16),
            pltpu.VMEM((tiles, text), F32),
            pltpu.VMEM((nh - 1, groups, 2, rows, HD), BF16),
            pltpu.VMEM((nh - 1, groups, 2, rows, HD), BF16),
            pltpu.VMEM((groups, rows, 2 * HD), F32),
            pltpu.VMEM((groups, nt, 2, rows, HD), BF16),
            pltpu.VMEM((HD + ONES, rows), BF16),
            pltpu.VMEM((slots, rows, text), F32),
            pltpu.VMEM((heads, HD, text), F32),
            pltpu.VMEM((heads, text), F32),
            pltpu.VMEM((heads, text), F32),
            pltpu.VMEM((groups, ni, 3, reps, text), F32),
            pltpu.VMEM((heads, text), F32),
            pltpu.VMEM((heads, text), F32),
            pltpu.VMEM((heads, text), F32),
            pltpu.VMEM((groups, nt - 1, 2, HD, rows), BF16),
            pltpu.VMEM((groups, nt + 1, 2, HD, rows), BF16),
            pltpu.VMEM((nt, 2, HD, rows), F32),
            pltpu.VMEM((nh, groups, 2, rows, HD), BF16),
            pltpu.VMEM((groups, half, gcols), BF16),
            pltpu.VMEM((groups, crosses, half, gcols), BF16),
            pltpu.VMEM((groups, crosses, half, gcols), BF16),
            dma((3,)), dma((nh, groups, 2)),
            dma((nh - 1, groups, 2)), dma((nh - 1, groups, 2)),
            dma((groups, 2, nt - 1)), dma((groups, 2)), dma((groups, nt, 2)),
            dma((groups, ni - 1)), dma((groups, ni - 1)),
            dma((groups,)), dma((groups,)),
            dma((groups, crosses)), dma((groups, crosses)),
            dma((groups,)), dma((groups,)),
            dma((groups, nt - 1, 2)), dma((groups, nt + 1, 2)),
            dma((nh - 1, groups, 2)), dma((nh - 1, groups, 2)),
        ],
        compiler_params=pltpu.CompilerParams(
            collective_id=0, has_side_effects=True, vmem_limit_bytes=VMEM_BUDGET
        ),
    )(image_feats, key_weight, value_weight, queries, grad_out, tile_image, text_sees)
    return (attn, grad_feats)


def solution(mesh):
    sizes = (mesh.shape["img"], mesh.shape["head"], mesh.shape["txt"])
    placed = (
        P(("img", "txt"), "head"),
        P("head", None),
        P("head", None),
        P("txt", "head"),
        P("txt", "head"),
        P("img"),
        P(),
    )
    return jax.shard_map(
        functools.partial(shards, sizes),
        mesh=mesh,
        in_specs=placed,
        out_specs=(P("txt", "head"), P(("img", "txt"), "head")),
        check_vma=False,
    )
```

```python
import functools
import math

import jax
import jax.numpy as jnp
from jax import lax
from jax.experimental import pallas as pl
from jax.experimental.pallas import tpu as pltpu
from jax.sharding import PartitionSpec as P

HD = 128
TILE = 128
TBLK = 128
MESH = pl.DeviceIdType.MESH
UNROLL = 8
LOG2E = 1.4426950408889634
NT = (((1,), (1,)), ((), ()))
F32 = jnp.float32
BF16 = jnp.bfloat16
HIDE = 2e30
FLOOR = -1e30
ONES = 16
VMEM_BUDGET = 58 * 1024 * 1024


def pick(index, table):
    value = jnp.int32(table[0])
    for at in range(1, len(table)):
        value = jnp.where(index == at, jnp.int32(table[at]), value)
    return value


def arrival_order(count):
    return [
        sorted((b for b in range(count) if b != z), key=lambda b: (abs(b - z), b))
        for z in range(count)
    ]


def departure_order(count):
    orders = []
    for z in range(count):
        above, below = list(range(count - 1, z, -1)), list(range(z))
        orders.append((above + below if 2 * z < count else below + above[::-1]) + [z])
    return orders


def kernel(
    sizes, keep,
    feats_hbm, kw_hbm, vw_hbm, q_hbm, g_hbm, tiles_hbm, sees_hbm,
    attn, dfeats,
    tile_image, text_sees, feats, kw, vw, qraw, graw, qt, gt, big, psend, precv, pacc, kvbuf, vtb, sbuf, numt, mst, tst,
    stbuf, lse, dlt, cown, gsend, grecv, gpart, hall, ocr, xs, xr,
    l_s, w_s, p_ss, p_rs, kv_ss, kv_fs, kv_rs, st_ss, st_rs, oc_ss, oc_rs, ox_ss, ox_rs,
    oa_ss, oa_rs, g_ss, g_rs, h_ss, h_rs,
):
    ni, nh, nt = sizes
    img, hd, txt = lax.axis_index("img"), lax.axis_index("head"), lax.axis_index("txt")
    rows, width = feats.shape
    groups = kvbuf.shape[0]
    own_cols = groups * HD
    text = qraw.shape[0]
    heads = qraw.shape[1] // HD
    reps = heads // groups
    block_tiles = rows // TILE
    scale = 1.0 / math.sqrt(HD)
    unroll = math.gcd(UNROLL, reps)
    half = text // 2
    gcols = reps * HD
    bits = ni.bit_length() - 1
    arrive, depart = arrival_order(nt), departure_order(nt)

    def cols_of(owner, group):
        return pl.ds(pl.multiple_of(owner * own_cols + group * HD, HD), HD)

    def other(step):
        return lax.rem(hd + step, nh)

    loads = [pltpu.make_async_copy(feats_hbm, feats, l_s.at[0])]
    weight_loads = {}
    for step in list(range(1, nh)) + [0]:
        for group in range(groups):
            cols = cols_of(other(step), group)
            pair = [
                pltpu.make_async_copy(src.at[:, cols], dst.at[:, cols], w_s.at[step, group, part])
                for part, (src, dst) in enumerate(((kw_hbm, kw), (vw_hbm, vw)))
            ]
            weight_loads[step, group] = pair
            loads += pair
    q_load = pltpu.make_async_copy(q_hbm, qraw, l_s.at[1])
    g_load = pltpu.make_async_copy(g_hbm, graw, l_s.at[2])
    tables = [
        pltpu.make_async_copy(tiles_hbm, tile_image, l_s.at[3]),
        pltpu.make_async_copy(sees_hbm, text_sees, l_s.at[4]),
    ]
    loads += [q_load, g_load] + tables
    for copy in loads:
        copy.start()

    barrier = pltpu.get_barrier_semaphore()
    for step in range(1, nh):
        pl.semaphore_signal(barrier, inc=1, device_id={"head": other(step)}, device_id_type=MESH)
    for step in range(1, nt):
        pl.semaphore_signal(barrier, inc=1, device_id={"txt": lax.rem(txt + step, nt)}, device_id_type=MESH)
    for step in range(1, ni):
        pl.semaphore_signal(barrier, inc=1, device_id={"img": lax.rem(img + step, ni)}, device_id_type=MESH)

    def remote(src, dst, ss, rs, axis, index):
        return pltpu.make_async_remote_copy(
            src_ref=src, dst_ref=dst, send_sem=ss, recv_sem=rs,
            device_id={axis: index}, device_id_type=MESH,
        )

    vtb[pl.ds(HD, ONES), :] = jnp.ones((ONES, rows), BF16)

    def project(step, group):
        for copy in weight_loads[step, group]:
            copy.wait()
        cols = cols_of(other(step), group)
        weights = jnp.concatenate([kw[:, cols], vw[:, cols]], axis=1)
        return jnp.dot(feats[...], weights, preferred_element_type=F32)

    loads[0].wait()
    p_copies = {}
    for step in range(1, nh):
        for group in range(groups):
            value = project(step, group).astype(BF16)
            if step == 1 and group == 0:
                pl.semaphore_wait(barrier, nh - 1 + nt - 1 + ni - 1)
            for part in range(2):
                psend[step - 1, group, part] = value[:, part * HD : (part + 1) * HD]
                at = (step - 1, group, part)
                copy = remote(
                    psend.at[at], precv.at[at], p_ss.at[at], p_rs.at[at], "head", other(step)
                )
                copy.start()
                p_copies[at] = copy
    for group in range(groups):
        pacc[group] = project(0, group)

    for copy in tables:
        copy.wait()
    first_block = txt * (text // TBLK)
    for tile in range(big.shape[0]):
        image = tile_image[tile]
        parts = [
            jnp.full((1, TBLK), text_sees[first_block + at, image].astype(F32))
            for at in range(text // TBLK)
        ]
        seen = jnp.concatenate(parts, axis=1)
        big[pl.ds(tile, 1), :] = jnp.where(seen > 0.5, 0.0, HIDE)

    def kv_copy(group, part, side):
        mine = kvbuf.at[group, txt, part]
        return remote(
            mine, mine, kv_ss.at[group, part, side], kv_rs.at[group, txt, part],
            "txt", txt + (1, -1)[side],
        )

    has_side = (txt < nt - 1, txt > 0)

    def own_sum(group, part):
        total = pacc[group, :, part * HD : (part + 1) * HD]
        for step in range(1, nh):
            p_copies[step - 1, group, part].wait_recv()
            total = total + precv[step - 1, group, part].astype(F32)
        kvbuf[group, txt, part] = total.astype(BF16)

    last_pass = [
        [max([0] + [s + 1 for s, b in enumerate(arrive[z]) if (b < z) == (side == 0)]) for z in range(nt)]
        for side in range(2)
    ]

    def send_own(group, after):
        for side in range(2):
            now = has_side[side]
            if after is not None:
                now = jnp.logical_and(now, pick(txt, last_pass[side]) == after)

            def go(side=side):
                for part in range(2):
                    kv_copy(group, part, side).start()

            pl.when(now)(go)

    def arrival(group, step):
        block = pick(txt, [arrive[z][step - 1] for z in range(nt)])
        onward = jnp.where(block < txt, txt + 1, txt - 1)
        valid = jnp.logical_and(onward >= 0, onward < nt)
        copies = []
        for part in range(2):
            there = kvbuf.at[group, block, part]
            copies.append(
                remote(
                    there, there, kv_fs.at[group, step, part], kv_rs.at[group, block, part],
                    "txt", onward,
                )
            )
        return block, valid, copies

    def receive(group, step):
        _, valid, copies = arrival(group, step)
        for copy in copies:
            copy.wait_recv()
            pl.when(valid)(copy.start)

    def pass_block(group, step):
        _, valid, copies = arrival(group, step)

        def go():
            for copy in copies:
                copy.wait_recv()
                copy.start()

        pl.when(valid)(go)

    def take(group, step):
        _, valid, copies = arrival(group, step)

        def go():
            for copy in copies:
                copy.wait_recv()

        pl.when(jnp.logical_not(valid))(go)

    def turn_over(group):
        def body(at, _):
            head = group * reps + at
            cols = pl.ds(pl.multiple_of(head * HD, HD), HD)
            qt[head] = qraw[:, cols].astype(F32).T.astype(BF16)
            gt[head] = graw[:, cols].astype(F32).T.astype(BF16)
            return 0

        lax.fori_loop(0, reps, body, 0)

    def scaled_scores(keys, head):
        return jnp.dot(keys, qt[head], preferred_element_type=F32) * (scale * LOG2E)

    def tiles_of(array):
        return [array[t * TILE : (t + 1) * TILE] for t in range(block_tiles)]

    def slot(group, block, at):
        return (group * nt + block) * reps + at

    def forward(group, block, first):
        vtb[pl.ds(0, HD), :] = kvbuf[group, block, 1].astype(F32).T.astype(BF16)

        def body(turn, _):
            at = [turn * unroll + i for i in range(unroll)]
            keys, values_t = kvbuf[group, block, 0], vtb[...]
            hide = [big[pl.ds(block * block_tiles + t, 1), :] for t in range(block_tiles)]
            kept, tops, totals, outs = [], [], [], []
            for i in range(unroll):
                head = group * reps + at[i]
                scores = scaled_scores(keys, head)
                if keep:
                    sbuf[slot(group, block, at[i])] = scores
                top = jnp.full((1, text), FLOOR, F32) if first else mst[pl.ds(head, 1), :]
                for t, part in enumerate(tiles_of(scores)):
                    top = jnp.maximum(top, jnp.max(part, axis=0, keepdims=True) - hide[t])
                kept.append(scores)
                tops.append(top)
            for i in range(unroll):
                head = group * reps + at[i]
                weights = jnp.concatenate(
                    [jnp.exp2(part - (tops[i] + hide[t])) for t, part in enumerate(tiles_of(kept[i]))],
                    axis=0,
                ).astype(BF16)
                both = jnp.dot(values_t, weights, preferred_element_type=F32)
                numer, total = both[:HD], both[HD : HD + 1]
                if not first:
                    shrink = jnp.exp2(mst[pl.ds(head, 1), :] - tops[i])
                    total = total + tst[pl.ds(head, 1), :] * shrink
                    numer = numer + numt[head] * shrink
                totals.append(total)
                outs.append(numer)
            for i in range(unroll):
                head = group * reps + at[i]
                mst[pl.ds(head, 1), :] = tops[i]
                tst[pl.ds(head, 1), :] = totals[i]
                numt[head] = outs[i]
            return 0

        lax.fori_loop(0, reps // unroll, body, 0)

    def group_rows(group):
        return pl.ds(group * reps, reps)

    def stats_copies(group):
        return [
            remote(
                stbuf.at[group, img], stbuf.at[group, img], st_ss.at[group, step - 1],
                st_rs.at[group, step - 1], "img", lax.rem(img + step, ni),
            )
            for step in range(1, ni)
        ]

    def stats_start(group):
        def deltas(at, _):
            head = group * reps + at
            stbuf[group, img, 2, pl.ds(at, 1), :] = jnp.sum(
                gt[head].astype(F32) * numt[head], axis=0, keepdims=True
            )
            return 0

        for at in range(reps):
            deltas(at, 0)
        stbuf[group, img, 0] = mst[group_rows(group), :]
        stbuf[group, img, 1] = tst[group_rows(group), :]
        for copy in stats_copies(group):
            copy.start()

    def stats_finish(group):
        for copy in stats_copies(group):
            copy.wait_recv()
        top = stbuf[group, 0, 0]
        for i in range(1, ni):
            top = jnp.maximum(top, stbuf[group, i, 0])
        total = jnp.zeros_like(top)
        delta = jnp.zeros_like(top)
        for i in range(ni):
            factor = jnp.exp2(stbuf[group, i, 0] - top)
            total = total + factor * stbuf[group, i, 1]
            delta = delta + factor * stbuf[group, i, 2]
        lse[group_rows(group), :] = top + jnp.log(total) * LOG2E
        dlt[group_rows(group), :] = delta / total
        cown[group_rows(group), :] = jnp.exp2(stbuf[group, img, 0] - top) / total

    def goal(step):
        return pick(txt, [depart[z][step] for z in range(nt)])

    def grad_copy(group, step, part):
        block = goal(step)
        up = block > txt
        target = jnp.where(up, txt + 1, txt - 1)
        back = jnp.where(up, txt - 1, txt + 1)
        lands = jnp.where(jnp.logical_and(target == block, jnp.logical_not(up)), nt, block)
        copy = remote(
            gsend.at[group, step, part], grecv.at[group, lands, part],
            g_ss.at[group, step, part], g_rs.at[group, lands, part], "txt", target,
        )
        relayed = jnp.logical_and(back >= 0, back < nt)
        return copy, relayed, block

    def grad_wait(group, place, part):
        remote(
            gsend.at[group, 0, part], grecv.at[group, place, part],
            g_ss.at[group, 0, part], g_rs.at[group, place, part], "txt", txt,
        ).wait_recv()

    def backward(group, step):
        block = goal(step)

        def body(turn, _):
            at = [turn * unroll + i for i in range(unroll)]
            keys, values = kvbuf[group, block, 0], kvbuf[group, block, 1]
            hide = [big[pl.ds(block * block_tiles + t, 1), :] for t in range(block_tiles)]
            probs_all, grads_all = [], []
            for i in range(unroll):
                head = group * reps + at[i]
                grad_probs = jnp.dot(values, gt[head], preferred_element_type=F32)
                if keep:
                    scores = sbuf[slot(group, block, at[i])]
                else:
                    scores = scaled_scores(keys, head)
                base = lse[pl.ds(head, 1), :]
                probs = jnp.concatenate(
                    [jnp.exp2(part - (base + hide[t])) for t, part in enumerate(tiles_of(scores))],
                    axis=0,
                )
                grads_all.append((probs * (grad_probs - dlt[pl.ds(head, 1), :])).astype(BF16))
                probs_all.append(probs.astype(BF16))
            picked = [group * reps + a for a in at]
            queries = jnp.concatenate([qt[head] for head in picked], axis=1)
            grads = jnp.concatenate([gt[head] for head in picked], axis=1)
            gpart[group, step, 0] = gpart[group, step, 0] + lax.dot_general(
                queries, jnp.concatenate(grads_all, axis=1), NT, preferred_element_type=F32
            )
            gpart[group, step, 1] = gpart[group, step, 1] + lax.dot_general(
                grads, jnp.concatenate(probs_all, axis=1), NT, preferred_element_type=F32
            )
            return 0

        gpart[group, step] = jnp.zeros((2, HD, rows), F32)
        lax.fori_loop(0, reps // unroll, body, 0)

    def grown(group, step, part):
        value = gpart[group, step, part]
        return value * scale if part == 0 else value

    def leave(group, step):
        for part in range(2):
            copy, relayed, _ = grad_copy(group, step, part)

            def go(copy=copy, part=part):
                gsend[group, step, part] = grown(group, step, part).astype(BF16)
                copy.start()

            pl.when(jnp.logical_not(relayed))(go)

    def pass_on(group, step):
        for part in range(2):
            copy, relayed, block = grad_copy(group, step, part)

            def go(copy=copy, part=part, block=block):
                grad_wait(group, block, part)
                gsend[group, step, part] = (
                    grown(group, step, part) + grecv[group, block, part].astype(F32)
                ).astype(BF16)
                copy.start()

            pl.when(relayed)(go)

    def h_copy(step, group, part):
        mine = hall.at[hd, group, part]
        at = (step - 1, group, part)
        return remote(mine, mine, h_ss.at[at], h_rs.at[at], "head", other(step))

    def own_grad(group):
        for part in range(2):
            gpart[group, nt - 1, part] = grown(group, nt - 1, part)
            for there, place in ((txt > 0, txt), (txt < nt - 1, jnp.int32(nt))):

                def add(place=place, part=part):
                    grad_wait(group, place, part)
                    gpart[group, nt - 1, part] = gpart[group, nt - 1, part] + grecv[group, place, part].astype(F32)

                pl.when(there)(add)
            hall[hd, group, part] = gpart[group, nt - 1, part].T.astype(BF16)
            for step in range(1, nh):
                h_copy(step, group, part).start()

    lower = lax.rem(img, 2)
    mate = img + 1 - 2 * lower
    mine_rows = pl.ds(pl.multiple_of(lower * half, half), half)
    mate_rows = pl.ds(pl.multiple_of((1 - lower) * half, half), half)

    def flip(bit):
        return img + (1 << bit) - (2 << bit) * lax.rem(img // (1 << bit), 2)

    def out_cols(group):
        return pl.ds(group * gcols, gcols)

    def pair_copy(group):
        return remote(
            qraw.at[mate_rows, out_cols(group)], ocr.at[group], oc_ss.at[group], oc_rs.at[group],
            "img", mate,
        )

    def cross_copy(group, bit):
        at = (group, bit - 1)
        return remote(xs.at[at], xr.at[at], ox_ss.at[at], ox_rs.at[at], "img", flip(bit))

    def share_copy(group):
        there = graw.at[mine_rows, out_cols(group)]
        return remote(there, there, oa_ss.at[group], oa_rs.at[group], "img", mate)

    def outputs(group):
        def body(at, _):
            head = group * reps + at
            cols = pl.ds(pl.multiple_of(head * HD, HD), HD)
            qraw[:, cols] = (numt[head] * cown[pl.ds(head, 1), :]).T.astype(BF16)
            return 0

        for at in range(reps):
            body(at, 0)
        pair_copy(group).start()

    def cross(group):
        pair_copy(group).wait_recv()
        total = qraw[mine_rows, out_cols(group)].astype(F32) + ocr[group].astype(F32)
        if bits > 1:
            xs[group, 0] = total.astype(BF16)
            cross_copy(group, 1).start()
        else:
            graw[mine_rows, out_cols(group)] = total.astype(BF16)
            share_copy(group).start()

    def share(group):
        for bit in range(1, bits):
            cross_copy(group, bit).wait_recv()
            total = (xs[group, bit - 1].astype(F32) + xr[group, bit - 1].astype(F32)).astype(BF16)
            if bit < bits - 1:
                xs[group, bit] = total
                cross_copy(group, bit + 1).start()
            else:
                graw[mine_rows, out_cols(group)] = total
                share_copy(group).start()

    def finish_output(group):
        share_copy(group).wait_recv()
        attn[:, out_cols(group)] = graw[:, out_cols(group)]

    per = math.gcd(width // text, 3)
    chunk = per * text

    def features(pairs, first, last):
        def body(at, _):
            span = pl.ds(pl.multiple_of(at * chunk, chunk), chunk)
            left = jnp.concatenate([hall[o, group, p] for o, group in pairs for p in range(2)], axis=1)
            right = jnp.concatenate(
                [w[span, cols_of(o, group)] for o, group in pairs for w in (kw, vw)], axis=1
            )
            value = lax.dot_general(left, right, NT, preferred_element_type=F32)
            for j in range(per):
                piece = value[:, j * text : (j + 1) * text]
                if not first:
                    piece = piece + sbuf[at * per + j]
                if last:
                    start = pl.multiple_of(at * chunk + j * text, text)
                    dfeats[:, pl.ds(start, text)] = piece.astype(BF16)
                else:
                    sbuf[at * per + j] = piece
            return 0

        lax.fori_loop(0, width // chunk, body, 0)

    def h_wait(group):
        for step in range(1, nh):
            for part in range(2):
                h_copy(step, group, part).wait_recv()

    for part in range(2):
        own_sum(0, part)

        def go(part=part, side=0):
            kv_copy(0, part, side).start()

        for side in range(2):
            pl.when(has_side[side])(functools.partial(go, part, side))
    q_load.wait()
    g_load.wait()
    turn_over(0)
    forward(0, txt, True)
    for part in range(2):
        own_sum(1, part)
    send_own(1, 0)
    pass_block(0, 1)
    send_own(1, 1)
    pass_block(0, 2)
    send_own(1, 2)
    take(0, 1)
    forward(0, arrival(0, 1)[0], False)
    turn_over(1)
    pass_block(0, 3)
    send_own(1, 3)
    take(0, 2)
    forward(0, arrival(0, 2)[0], False)
    take(0, 3)
    forward(0, arrival(0, 3)[0], False)
    stats_start(0)
    forward(1, txt, True)
    pass_block(1, 1)
    stats_finish(0)
    backward(0, 0)
    leave(0, 0)
    pass_block(1, 2)
    take(1, 1)
    forward(1, arrival(1, 1)[0], False)
    backward(0, 1)
    leave(0, 1)
    pass_block(1, 3)
    pass_on(0, 0)
    take(1, 2)
    forward(1, arrival(1, 2)[0], False)
    take(1, 3)
    forward(1, arrival(1, 3)[0], False)
    stats_start(1)
    backward(0, 2)
    leave(0, 2)
    pass_on(0, 1)
    outputs(0)
    stats_finish(1)
    backward(1, 0)
    leave(1, 0)
    cross(0)
    pass_on(0, 2)
    backward(1, 1)
    leave(1, 1)
    backward(0, 3)
    backward(1, 2)
    leave(1, 2)
    outputs(1)
    pass_on(1, 0)
    cross(1)
    backward(1, 3)
    own_grad(0)
    pass_on(1, 1)
    pass_on(1, 2)
    share(0)
    h_wait(0)
    owners = [hd] + [other(step) for step in range(1, nh)]
    features([(o, 0) for o in owners], True, False)
    share(1)
    own_grad(1)
    features([(hd, 1)], False, False)
    finish_output(0)
    finish_output(1)
    h_wait(1)
    features([(o, 1) for o in owners[1:]], False, True)

    for copy in p_copies.values():
        copy.wait_send()
    for group in range(groups):
        for side in range(2):

            def own_sent(group=group, side=side):
                for part in range(2):
                    kv_copy(group, part, side).wait_send()

            pl.when(has_side[side])(own_sent)
        for step in range(1, nt):
            _, valid, copies = arrival(group, step)

            def passed(copies=copies):
                for copy in copies:
                    copy.wait_send()

            pl.when(valid)(passed)
        for copy in stats_copies(group):
            copy.wait_send()
        for step in range(nt - 1):
            for part in range(2):
                grad_copy(group, step, part)[0].wait_send()
        pair_copy(group).wait_send()
        for bit in range(1, bits):
            cross_copy(group, bit).wait_send()
        share_copy(group).wait_send()
        for step in range(1, nh):
            for part in range(2):
                h_copy(step, group, part).wait_send()


def flush(attn_ready, feats_ready, attn, feats, sems):
    copies = [
        pltpu.make_async_copy(attn_ready, attn, sems.at[0]),
        pltpu.make_async_copy(feats_ready, feats, sems.at[1]),
    ]
    for copy in copies:
        copy.start()
    for copy in copies:
        copy.wait()


def shards(sizes, image_feats, key_weight, value_weight, queries, grad_out, tile_image, text_sees):
    ni, nh, nt = sizes
    rows, feat_width = image_feats.shape
    text, width = queries.shape
    heads = width // HD
    own_cols = key_weight.shape[1] // nh
    groups = own_cols // HD
    reps = heads // groups
    half = text // 2
    gcols = reps * HD
    tiles = nt * rows // TILE
    crosses = max(ni.bit_length() - 2, 1)
    slots = feat_width // text
    keep = nt * heads * rows * text * 4 <= VMEM_BUDGET // 3
    if keep:
        slots = max(slots, nt * heads)
    dma = pltpu.SemaphoreType.DMA
    hbm = pl.BlockSpec(memory_space=pl.ANY)
    vmem = pl.BlockSpec(memory_space=pltpu.VMEM)
    attn, grad_feats = pl.pallas_call(
        functools.partial(kernel, sizes, keep),
        out_shape=(
            pltpu.VMEM((text, width), BF16),
            pltpu.VMEM(image_feats.shape, BF16),
        ),
        in_specs=[hbm] * 7,
        out_specs=(vmem, vmem),
        scratch_shapes=[
            pltpu.SMEM(tile_image.shape, tile_image.dtype),
            pltpu.SMEM(text_sees.shape, text_sees.dtype),
            pltpu.VMEM(image_feats.shape, BF16),
            pltpu.VMEM(key_weight.shape, BF16),
            pltpu.VMEM(value_weight.shape, BF16),
            pltpu.VMEM((text, width), BF16),
            pltpu.VMEM((text, width), BF16),
            pltpu.VMEM((heads, HD, text), BF16),
            pltpu.VMEM((heads, HD, text), BF16),
            pltpu.VMEM((tiles, text), F32),
            pltpu.VMEM((nh - 1, groups, 2, rows, HD), BF16),
            pltpu.VMEM((nh - 1, groups, 2, rows, HD), BF16),
            pltpu.VMEM((groups, rows, 2 * HD), F32),
            pltpu.VMEM((groups, nt, 2, rows, HD), BF16),
            pltpu.VMEM((HD + ONES, rows), BF16),
            pltpu.VMEM((slots, rows, text), F32),
            pltpu.VMEM((heads, HD, text), F32),
            pltpu.VMEM((heads, text), F32),
            pltpu.VMEM((heads, text), F32),
            pltpu.VMEM((groups, ni, 3, reps, text), F32),
            pltpu.VMEM((heads, text), F32),
            pltpu.VMEM((heads, text), F32),
            pltpu.VMEM((heads, text), F32),
            pltpu.VMEM((groups, nt - 1, 2, HD, rows), BF16),
            pltpu.VMEM((groups, nt + 1, 2, HD, rows), BF16),
            pltpu.VMEM((groups, nt, 2, HD, rows), F32),
            pltpu.VMEM((nh, groups, 2, rows, HD), BF16),
            pltpu.VMEM((groups, half, gcols), BF16),
            pltpu.VMEM((groups, crosses, half, gcols), BF16),
            pltpu.VMEM((groups, crosses, half, gcols), BF16),
            dma((5,)), dma((nh, groups, 2)),
            dma((nh - 1, groups, 2)), dma((nh - 1, groups, 2)),
            dma((groups, 2, 2)), dma((groups, nt, 2)), dma((groups, nt, 2)),
            dma((groups, ni - 1)), dma((groups, ni - 1)),
            dma((groups,)), dma((groups,)),
            dma((groups, crosses)), dma((groups, crosses)),
            dma((groups,)), dma((groups,)),
            dma((groups, nt - 1, 2)), dma((groups, nt + 1, 2)),
            dma((nh - 1, groups, 2)), dma((nh - 1, groups, 2)),
        ],
        compiler_params=pltpu.CompilerParams(
            collective_id=0, has_side_effects=True, vmem_limit_bytes=VMEM_BUDGET
        ),
    )(image_feats, key_weight, value_weight, queries, grad_out, tile_image, text_sees)
    return pl.pallas_call(
        flush,
        out_shape=(
            jax.ShapeDtypeStruct((text, width), BF16),
            jax.ShapeDtypeStruct(image_feats.shape, BF16),
        ),
        in_specs=[hbm] * 2,
        out_specs=(hbm, hbm),
        scratch_shapes=[dma((2,))],
    )(
        pltpu.with_memory_space_constraint(attn, pltpu.VMEM),
        pltpu.with_memory_space_constraint(grad_feats, pltpu.VMEM),
    )


def solution(mesh):
    sizes = (mesh.shape["img"], mesh.shape["head"], mesh.shape["txt"])
    placed = (
        P(("img", "txt"), "head"),
        P("head", None),
        P("head", None),
        P("txt", "head"),
        P("txt", "head"),
        P("img"),
        P(),
    )
    return jax.shard_map(
        functools.partial(shards, sizes),
        mesh=mesh,
        in_specs=placed,
        out_specs=(P("txt", "head"), P(("img", "txt"), "head")),
        check_vma=False,
    )
```
